512 devices in a mesh: dp: 16 (over z, x_lo), expert: 32 (over x_hi, y, core).
Axes of the slice: x: 4 (x_hi: 2, x_lo: 2; x = x_hi * 2 + x_lo), y: 8, z: 8, core: 2. Of those that a mesh axis runs over, the one named last changes fastest.
Arguments:
- tokens: bfloat16 [1024, 2048], P('expert', 'dp'), may hold values from -6 to 6
- routes: int32 [1024, 8], P('expert'), may hold values from 0 to 127, all different within a row; in each aligned block of 32 rows (0 to 31, 32 to 63, ...) at most 4 rows name the same one
- route_weight: float32 [1024, 8], P('expert'), may hold values from 0.05 to 0.5
- gate_weight: bfloat16 [128, 2048, 768], P('expert', 'dp'), may hold values from -0.125 to 0.125
- up_weight: bfloat16 [128, 2048, 768], P('expert', 'dp'), may hold values from -0.125 to 0.125
- down_weight: bfloat16 [128, 768, 2048], P('expert', None, 'dp'), may hold values from -0.21875 to 0.21875
- trained_down: float32 [128, 768, 2048], P('expert', 'dp'), may hold values from -0.21875 to 0.21875
Outputs:
- mixed: bfloat16 [1024, 2048], P('expert', 'dp')
- synced_down: bfloat16 [128, 768, 2048], P('expert', None, 'dp')
The draws below stay inside these ranges and needn't reach their ends.
Inputs may be any that keep to these rules, and one draw needn't show every extreme that they name: `routes`: each row names 8 different experts. Among the 32 rows of one device (aligned blocks), no expert is named more than 4 times, a bound that some block reaches.
All inputs are finite; a program needn't handle non-finite values.
Results may differ from the reference program's by a relative error of at most 0.0058.
Values may be sent and summed in bfloat16 or wider, within the bound.
A program may use at most 64 MiB of HBM per device.

```python
import math
import jax
import jax.numpy as jnp
import numpy as np
from jax import lax

D = 2048
FF = 768
TOP = 8
EXPERTS = 128
TOK_DEV = 32
CAP = 4
TOKENS = 1024


def level_of(stream_key, extent, pieces, least, high):
    loudness = 1.0
    for dim, parts in pieces:
        heights = jax.random.uniform(jax.random.fold_in(jax.random.fold_in(stream_key, 6), dim), (parts,), jnp.float32, least / len(pieces), high / len(pieces))
        loudness = loudness * jnp.repeat(jnp.exp(heights), extent[dim] // parts).reshape((-1,) + (1,) * (len(extent) - 1 - dim))
    return loudness


def routed_block(key, own, number, rows, amount, top, limit, lean):
    order = jax.random.permutation(key, amount)
    crowded, common = shares(amount, rows * top, limit, lean, True), shares(amount, rows * top, limit, lean, False)
    places = jnp.arange(amount)

    def named(lengths, turn):
        used = int((lengths > 0).sum())
        fixed = max(1, used // 4)
        shifted = fixed + (places - fixed + turn * (used - fixed)) % max(1, amount - fixed)
        return jnp.zeros((amount,), jnp.int32).at[order[jnp.where(places < fixed, places, shifted)]].set(jnp.asarray(lengths, jnp.int32))

    lengths = jnp.where(number % 4 == 0, named(crowded, number // 4), named(common, number - number // 4 - 1))
    mixed = jax.random.permutation(jax.random.fold_in(own, 3), amount)
    giver, receiver = mixed[0:amount // 2 * 2:2], mixed[1:amount // 2 * 2:2]
    margin = jnp.minimum(lengths[giver] - 1, limit - lengths[receiver]) // 2
    margin = jnp.where((giver == order[0]) | (receiver == order[0]) | (lengths[receiver] == 0), 0, jnp.maximum(margin, 0))
    shifted = jax.random.randint(jax.random.fold_in(own, 4), (amount // 2,), 0, 1 << 20) % (margin + 1)
    lengths = lengths.at[giver].add(-shifted).at[receiver].add(shifted)
    items = jnp.searchsorted(jnp.cumsum(lengths), jnp.arange(rows * top), side="right").astype(jnp.int32)
    grid = items.reshape(top, rows).T
    grid = grid[jax.random.permutation(jax.random.fold_in(own, 1), rows)]
    turn = jax.random.randint(jax.random.fold_in(own, 2), (rows, 1), 0, top)
    return jnp.take_along_axis(grid, (jnp.arange(top)[None, :] + turn) % top, axis=1)


def shares(number_of, total, most, slope, full):
    loads = [(1 << 20) // math.isqrt(standing ** slope) + 1 for standing in range(1, number_of + 1)]
    largest = most if full else min(most, max(-(-total // number_of), total * loads[0] // sum(loads)))
    least = 1 if total - largest >= number_of - 1 else 0
    given, spare = [largest] + [least] * (number_of - 1), total - largest - least * (number_of - 1)
    while spare > 0:
        movable = [i for i in range(1, number_of) if given[i] < largest] or [i for i in range(1, number_of) if given[i] < most]
        pool, remaining = sum([loads[i] for i in movable]), spare
        for i in movable:
            addition = min(most - given[i], max(1, remaining * loads[i] // pool), spare)
            given[i] = given[i] + addition
            spare = spare - addition
    return np.array(given)


def noise(key, extent, width, reach, split=(), kind=jnp.bfloat16):
    loudness = level_of(key, extent, split, -0.22, 0.18) if split else 1.0
    drawn = jax.random.normal(key, extent, jnp.float32) * width * loudness
    return jnp.minimum(jnp.maximum(drawn, -reach), reach).astype(kind)


def setup_inputs(seed: int = 0) -> dict:
    key_list = jax.random.split(jax.random.key(seed), 8)
    tokens = noise(key_list[0], (TOKENS, D), 1.0, 6.0, ((0, 32), (1, 16)))
    routes_keys = jax.random.split(jax.random.fold_in(key_list[1], 1), TOKENS // TOK_DEV)
    routes_turns = jax.random.permutation(jax.random.fold_in(key_list[1], 3), TOKENS // TOK_DEV)
    routes = jax.vmap(lambda own, number: routed_block(jax.random.fold_in(key_list[1], 2), own, number, TOK_DEV, EXPERTS, TOP, CAP, 2))(routes_keys, routes_turns).reshape((TOKENS, TOP))
    route_weight = jnp.clip(jnp.exp(math.log(0.5) - 2.3025851 * jax.random.uniform(key_list[2], (TOKENS, TOP), jnp.float32) ** level_of(key_list[2], (TOKENS, TOP), ((0, 32),), -0.2, 0.2)), 0.05, 0.5)
    gate_weight = noise(key_list[3], (EXPERTS, D, FF), D ** -0.5, 0.125, ((0, 32), (1, 16)))
    up_weight = noise(key_list[4], (EXPERTS, D, FF), D ** -0.5, 0.125, ((0, 32), (1, 16)))
    down_weight = noise(key_list[5], (EXPERTS, FF, D), FF ** -0.5, 0.21875, ((0, 32), (2, 16)))
    trained_down = noise(key_list[6], (EXPERTS, FF, D), FF ** -0.5, 0.21875, ((0, 32), (1, 16)), jnp.float32)
    return {"tokens": tokens, "routes": routes, "route_weight": route_weight, "gate_weight": gate_weight, "up_weight": up_weight, "down_weight": down_weight, "trained_down": trained_down}


def reference(tokens, routes, route_weight, gate_weight, up_weight, down_weight, trained_down):
    blocks = TOKENS // TOK_DEV
    labels = jnp.arange(EXPERTS, dtype=jnp.int32)
    counts = jnp.sum((routes[:, :, None] == labels[None, None, :]).astype(jnp.int32), axis=1)
    per_block = counts.reshape(blocks, TOK_DEV, EXPERTS)
    earlier = (jnp.cumsum(per_block, axis=1) - per_block).reshape(TOKENS, EXPERTS).astype(jnp.int32)
    slot_index = jnp.take_along_axis(earlier, routes, axis=1).astype(jnp.int32)
    block_of = (jnp.arange(TOKENS, dtype=jnp.int32) // TOK_DEV)[:, None]
    position = (block_of * CAP + slot_index).astype(jnp.int32)
    rows_expert = blocks * CAP
    token_ids = jnp.broadcast_to(jnp.arange(TOKENS, dtype=jnp.int32)[:, None], routes.shape)
    row_table = jnp.full((EXPERTS, rows_expert), TOKENS, jnp.int32).at[routes, position].set(token_ids)
    padded = jnp.concatenate([tokens, jnp.zeros((1, D), tokens.dtype)], axis=0)

    def one_expert(operands):
        row_index, gate_mat, up_mat, down_mat = operands
        gathered = padded[row_index]
        gate_pre = jnp.dot(gathered, gate_mat, preferred_element_type=jnp.float32)
        up_pre = jnp.dot(gathered, up_mat, preferred_element_type=jnp.float32)
        hidden = (jax.nn.silu(gate_pre) * up_pre).astype(jnp.bfloat16)
        return jnp.dot(hidden, down_mat, preferred_element_type=jnp.float32).astype(jnp.bfloat16)

    results = lax.map(one_expert, (row_table, gate_weight, up_weight, down_weight))
    picked = results[routes, position]
    mixed = jnp.sum(route_weight[:, :, None] * picked.astype(jnp.float32), axis=1).astype(jnp.bfloat16)
    return mixed, trained_down.astype(jnp.bfloat16)
```

```python
import functools

import jax
import jax.numpy as jnp
from jax import lax
from jax.experimental import pallas as pl
from jax.experimental.pallas import tpu as pltpu
from jax.sharding import Mesh
from jax.sharding import PartitionSpec as P

DP = ("z", "xl")
BF = jnp.bfloat16
F32 = jnp.float32


def dot(a, b, precision=None):
    return jnp.dot(a, b, preferred_element_type=F32, precision=precision)


def silu(v):
    return v / (1.0 + jnp.exp(-v))


def kernel(
    tokens, routes, route_weight, gate, up, down, trained,
    mixed, synced,
    out_tok, arr, wg, wu, wd, psend, precv, hid, oute, ret, td, td_send,
    load_sem, w_send, w_recv, d_send, d_recv, p_send, p_recv, h_send, h_recv, e_send, e_recv, a_send, a_recv,
):
    z, xl, g = lax.axis_index("z"), lax.axis_index("xl"), lax.axis_index("expert")
    other = 1 - xl
    seat = g * 2 + xl
    rank = z * 2 + xl
    TOK, WIDTH = tokens.shape
    FF = gate.shape[2]

    def at(z_, xl_, g_):
        return dict(device_id={"z": z_, "xl": xl_, "expert": g_}, device_id_type=pl.DeviceIdType.MESH)

    load_td = pltpu.make_async_copy(trained, td, load_sem.at[0])
    load_td.start()
    loads = []
    here = pl.ds(pl.multiple_of(128 * xl, 128), 128)
    for e in range(2):
        for n, (src, dst) in enumerate(((gate, wg), (up, wu))):
            loads.append(pltpu.make_async_copy(src.at[2 * xl + e], dst.at[e, here], load_sem.at[1 + 2 * e + n]))
    for e in range(2):
        loads.append(pltpu.make_async_copy(down.at[2 * xl + e], wd.at[e, :, here], load_sem.at[5 + e]))
    for load in loads:
        load.start()

    barrier = pltpu.get_barrier_semaphore()

    @pl.loop(1, 64)
    def _(i):
        peer = lax.rem(seat + i, 64)
        pl.semaphore_signal(barrier, inc=1, **at(z, lax.rem(peer, 2), lax.div(peer, 2)))

    @pl.loop(1, 8)
    def _(i):
        peer = lax.rem(z + i, 8)
        pl.semaphore_signal(barrier, inc=1, **at(peer, xl, g))
        pl.semaphore_signal(barrier, inc=1, **at(peer, other, g))

    slots = 512
    row = lax.broadcasted_iota(jnp.int32, (TOK, slots), 1)
    chosen = jnp.zeros((TOK, slots), F32)
    weight = jnp.zeros((TOK, slots), F32)
    for k in range(8):
        hit = routes[:, k : k + 1] == lax.shift_right_logical(row, 2)
        chosen = jnp.where(hit, 1.0, chosen)
        weight = jnp.where(hit, route_weight[:, k : k + 1], weight)
    before = lax.broadcasted_iota(jnp.int32, (TOK, TOK), 1) < lax.broadcasted_iota(jnp.int32, (TOK, TOK), 0)
    earlier = dot(jnp.where(before, 1.0, 0.0).astype(BF), chosen.astype(BF))
    slot = lax.bitwise_and(row, 3).astype(F32)
    placed = jnp.where((chosen > 0.5) & (earlier == slot), 1.0, 0.0)
    combine = placed * weight
    outgoing = lax.dot_general(
        placed.astype(BF), tokens[...], (((0,), (0,)), ((), ())), preferred_element_type=F32
    ).astype(BF)
    out_tok[...] = outgoing.reshape(64, 8, WIDTH)
    arr[xl * 32 + g] = out_tok[seat]

    load_td.wait()
    for r in range(16):
        td_send[r] = td[:, :, 128 * r : 128 * r + 128].astype(BF)

    pl.semaphore_wait(barrier, 77)

    @pl.loop(1, 64)
    def _(i):
        peer = lax.rem(seat + i, 64)
        pltpu.make_async_remote_copy(
            out_tok.at[peer], arr.at[xl * 32 + g], d_send, d_recv, **at(z, lax.rem(peer, 2), lax.div(peer, 2))
        ).start()

    sends = []
    for e in range(2):
        for n, (src, dst) in enumerate(((gate, wg), (up, wu))):
            sends.append(pltpu.make_async_remote_copy(
                src.at[2 * other + e], dst.at[e, here], w_send.at[2 * e + n], w_recv.at[2 * e + n], **at(z, other, g)))
    for e in range(2):
        sends.append(pltpu.make_async_remote_copy(
            down.at[2 * other + e], wd.at[e, :, here], w_send.at[4 + e], w_recv.at[4 + e], **at(z, other, g)))
    for send in sends:
        send.start()

    mine = pl.ds(pl.multiple_of(48 * rank, 16), 48)

    def sync_to(z_, xl_):
        return pltpu.make_async_remote_copy(
            td_send.at[z_ * 2 + xl_], synced.at[:, mine], a_send, a_recv, **at(z_, xl_, g))

    own = pltpu.make_async_copy(td_send.at[rank], synced.at[:, mine], load_sem.at[7])
    own.start()

    @pl.loop(1, 8)
    def _(i):
        sync_to(lax.rem(z + i, 8), xl).start()

    def waited(buf, count, sem):
        return pltpu.make_async_copy(buf.at[pl.ds(0, count)], buf.at[pl.ds(0, count)], sem)

    waited(arr, 63, d_recv).wait()
    x = jnp.concatenate([arr[0:32].reshape(256, WIDTH), arr[32:64].reshape(256, WIDTH)], axis=1)
    r0 = lax.broadcasted_iota(jnp.int32, (256, 256), 0)
    r1 = lax.broadcasted_iota(jnp.int32, (256, 256), 1)

    def grouped(r):
        return (lax.bitwise_and(lax.shift_right_logical(r, 2), 31) * 8
                + lax.shift_right_logical(r, 7) * 4 + lax.bitwise_and(r, 3))

    order = jnp.where(grouped(r0) == r1, 1.0, 0.0).astype(BF)
    back = jnp.where(grouped(r1) == r0, 1.0, 0.0).astype(BF)
    x = dot(order, x).astype(BF)

    for e in range(2):
        xe = x[128 * e : 128 * e + 128]
        for n, w in enumerate((wg, wu)):
            loads[2 * e + n].wait()
            sends[2 * e + n].wait_recv()
            psend[e, :, n] = dot(xe, w[e]).astype(BF).reshape(8, 16, FF)
        precv[e, z] = psend[e, z]

        @pl.loop(1, 8)
        def _(i):
            peer = lax.rem(z + i, 8)
            pltpu.make_async_remote_copy(
                psend.at[e, peer], precv.at[e, z], p_send.at[e], p_recv.at[e], **at(peer, xl, g)).start()

    for e in range(2):
        waited(precv.at[e], 7, p_recv.at[e]).wait()
        total = precv[e, 0].astype(F32)
        for s in range(1, 8):
            total = total + precv[e, s].astype(F32)
        hid[e, z] = (silu(total[0]) * total[1]).astype(BF)

        @pl.loop(1, 8)
        def _(i):
            peer = lax.rem(z + i, 8)
            pltpu.make_async_remote_copy(
                hid.at[e, z], hid.at[e, z], h_send.at[e], h_recv.at[e], **at(peer, xl, g)).start()

    sync_to(z, other).start()

    @pl.loop(1, 8)
    def _(i):
        sync_to(lax.rem(z + i, 8), other).start()

    outs = []
    for e in range(2):
        loads[4 + e].wait()
        sends[4 + e].wait_recv()
        waited(hid.at[e], 7, h_recv.at[e]).wait()
        outs.append(dot(hid[e].reshape(128, FF), wd[e]).astype(BF))
    out = dot(back, jnp.concatenate(outs, axis=0)).astype(BF)
    for n in range(2):
        oute[32 * n : 32 * n + 32] = out[:, 128 * n : 128 * n + 128].reshape(32, 8, WIDTH)
    ret[seat] = oute[xl * 32 + g]

    @pl.loop(1, 64)
    def _(i):
        peer = lax.rem(seat + i, 64)
        px, pg = lax.rem(peer, 2), lax.div(peer, 2)
        pltpu.make_async_remote_copy(
            oute.at[px * 32 + pg], ret.at[seat], e_send, e_recv, **at(z, px, pg)).start()

    waited(ret, 63, e_recv).wait()
    mixed[...] = dot(
        combine, ret[...].reshape(slots, WIDTH).astype(F32), precision=lax.Precision.HIGHEST
    ).astype(BF)

    own.wait()
    pltpu.make_async_copy(td_send.at[pl.ds(0, 15)], td_send.at[pl.ds(0, 15)], a_recv).wait()
    pltpu.make_async_copy(td_send.at[pl.ds(0, 15)], td_send.at[pl.ds(0, 15)], a_send).wait()
    waited(out_tok, 63, d_send).wait()
    waited(oute, 63, e_send).wait()
    for e in range(2):
        waited(psend.at[e], 7, p_send.at[e]).wait()
        waited(hid.at[e], 7, h_send.at[e]).wait()
    for send in sends:
        send.wait_send()


def local(tokens, routes, route_weight, gate, up, down, trained):
    V, A = pl.BlockSpec(memory_space=pltpu.VMEM), pl.BlockSpec(memory_space=pl.ANY)
    dma = pltpu.SemaphoreType.DMA
    FF = gate.shape[2]
    return pl.pallas_call(
        kernel,
        out_shape=(
            jax.ShapeDtypeStruct(tokens.shape, BF),
            jax.ShapeDtypeStruct(down.shape, BF),
        ),
        in_specs=[V, V, V, A, A, A, A],
        out_specs=(V, A),
        scratch_shapes=[
            pltpu.VMEM((64, 8, 128), BF),
            pltpu.VMEM((64, 8, 128), BF),
            pltpu.VMEM((2, 256, FF), BF),
            pltpu.VMEM((2, 256, FF), BF),
            pltpu.VMEM((2, FF, 256), BF),
            pltpu.VMEM((2, 8, 2, 16, FF), BF),
            pltpu.VMEM((2, 8, 2, 16, FF), BF),
            pltpu.VMEM((2, 8, 16, FF), BF),
            pltpu.VMEM((64, 8, 128), BF),
            pltpu.VMEM((64, 8, 128), BF),
            pltpu.VMEM(trained.shape, F32),
            pltpu.VMEM((16, 4, 48, 128), BF),
            dma((8,)), dma((6,)), dma((6,)), dma, dma, dma((2,)), dma((2,)), dma((2,)), dma((2,)), dma, dma, dma, dma,
        ],
        compiler_params=pltpu.CompilerParams(collective_id=0, has_side_effects=True),
        name="moe_step",
    )(tokens, routes, route_weight, gate, up, down, trained)


def solution(mesh):
    torus = Mesh(mesh.devices.reshape(8, 2, mesh.shape["expert"]), ("z", "xl", "expert"))
    placed = (
        P("expert", DP),
        P("expert", None),
        P("expert", None),
        P("expert", DP, None),
        P("expert", DP, None),
        P("expert", None, DP),
        P("expert", DP, None),
    )
    return jax.shard_map(
        local,
        mesh=torus,
        in_specs=placed,
        out_specs=(P("expert", DP), P("expert", None, DP)),
        check_vma=False,
    )
```

```python
import jax
import jax.numpy as jnp
from jax import lax
from jax.experimental import pallas as pl
from jax.experimental.pallas import tpu as pltpu
from jax.sharding import Mesh
from jax.sharding import PartitionSpec as P

DP = ("z", "xl")
BF = jnp.bfloat16
F32 = jnp.float32
CHUNKS = 4
AWAY = sorted(
    ((dy, flip) for dy in range(8) for flip in range(8) if dy or flip),
    key=lambda a: -(min(a[0], 8 - a[0]) + (a[1] >> 2) * 2 * (1 - (a[1] & 1)) + (a[1] & 1)),
)
ZAWAY = (4, 3, 5, 2, 6, 1, 7)
FAR = ZAWAY + (0,)
DIRECT = (3,)
EARLY = 3
ORDER = (0, 1, 10, 2, 11, 20, 3, 12, 21, 30, 13, 22, 31, 23, 32, 33)


def dot(a, b, precision=None):
    return jnp.dot(a, b, preferred_element_type=F32, precision=precision)


def silu(v):
    return v / (1.0 + jnp.exp(-v))


def kernel(
    tokens_hbm, routes_hbm, route_weight_hbm, gate, up, down, trained,
    mixed, synced,
    tokens, routes, route_weight, out_tok, arr, wgu, wd, psend, precv, pagg, hid, oute, ret, td, td_send, td_relay, combine,
    load_sem, w_send, w_recv, d_send, d_recv, p_send, p_recv, h_send, h_recv, e_send, e_recv, a_send, a_recv,
    x_send, x_recv, b_send, b_recv, r_recv, f_recv,
):
    z, xl, g = lax.axis_index("z"), lax.axis_index("xl"), lax.axis_index("expert")
    other = 1 - xl
    seat = g * 2 + xl
    rank = z * 2 + xl
    TOK, WIDTH = tokens.shape
    FF = gate.shape[2]
    PART = FF // 2

    def at(z_, xl_, g_):
        return dict(device_id={"z": z_, "xl": xl_, "expert": g_}, device_id_type=pl.DeviceIdType.MESH)

    def away(dy, flip):
        y = lax.bitwise_and(g + 2 * dy, 14)
        high = lax.bitwise_and(g, 16)
        high = 16 - high if flip & 4 else high
        core = lax.bitwise_and(g, 1)
        core = 1 - core if flip & 2 else core
        return (other if flip & 1 else xl), high + y + core

    def along(dz):
        return lax.bitwise_and(z + dz, 7)

    small = [
        pltpu.make_async_copy(a, b, load_sem.at[n])
        for n, (a, b) in enumerate(((routes_hbm, routes), (route_weight_hbm, route_weight), (tokens_hbm, tokens)))
    ]
    for load in small:
        load.start()

    with jax.named_scope("signals"):
        barrier = pltpu.get_barrier_semaphore()
        for dy, flip in AWAY:
            px, pg = away(dy, flip)
            pl.semaphore_signal(barrier, inc=1, **at(z, px, pg))
        for dz in ZAWAY:
            pl.semaphore_signal(barrier, inc=1, **at(along(dz), xl, g))

    load_td = pltpu.make_async_copy(trained, td, load_sem.at[3])
    load_td.start()
    here = pl.ds(pl.multiple_of(128 * xl, 128), 128)
    loads, sends = [], []
    for c in range(CHUNKS):
        e, half = c // 2, c % 2
        for n, src in enumerate((gate, up)):
            cols = pl.ds(PART * half, PART)
            dst = wgu.at[c, here, pl.ds(PART * n, PART)]
            loads.append(pltpu.make_async_copy(src.at[2 * xl + e, :, cols], dst, load_sem.at[4 + 2 * c + n]))
            sends.append(pltpu.make_async_remote_copy(
                src.at[2 * other + e, :, cols], dst, w_send.at[2 * c + n], w_recv.at[2 * c + n], **at(z, other, g)))
    for e in range(2):
        dst = wd.at[e, :, here]
        loads.append(pltpu.make_async_copy(down.at[2 * xl + e], dst, load_sem.at[12 + e]))
        sends.append(pltpu.make_async_remote_copy(
            down.at[2 * other + e], dst, w_send.at[8 + e], w_recv.at[8 + e], **at(z, other, g)))
    for load in loads:
        load.start()

    with jax.named_scope("routing"):
        for load in small:
            load.wait()
        slots = 512
        row = lax.broadcasted_iota(jnp.int32, (slots, TOK), 0)
        chosen = jnp.zeros((slots, TOK), F32)
        weight = jnp.zeros((slots, TOK), F32)
        for k in range(8):
            hit = routes[k : k + 1, :] == lax.shift_right_logical(row, 2)
            chosen = jnp.where(hit, 1.0, chosen)
            weight = jnp.where(hit, route_weight[k : k + 1, :], weight)
        before = lax.broadcasted_iota(jnp.int32, (TOK, TOK), 0) < lax.broadcasted_iota(jnp.int32, (TOK, TOK), 1)
        earlier = dot(chosen.astype(BF), jnp.where(before, 1.0, 0.0).astype(BF))
        slot = lax.bitwise_and(row, 3).astype(F32)
        placed = jnp.where((chosen > 0.5) & (earlier == slot), 1.0, 0.0)
        combine[...] = placed * weight
        out_tok[...] = dot(placed.astype(BF), tokens[...]).astype(BF).reshape(64, 8, WIDTH)
        arr[xl * 32 + g] = out_tok[seat]

    with jax.named_scope("barrier"):
        pl.semaphore_wait(barrier, 70)

    with jax.named_scope("issue"):
        for dy, flip in AWAY:
            px, pg = away(dy, flip)
            pltpu.make_async_remote_copy(
                out_tok.at[pg * 2 + px], arr.at[xl * 32 + g], d_send, d_recv, **at(z, px, pg)).start()
        for send in sends:
            send.start()

    with jax.named_scope("cast"):
        load_td.wait()
        for r in range(16):
            td_send[r // 2, r % 2] = td[:, :, 128 * r : 128 * r + 128].astype(BF)

    def rows_of(r):
        return pl.ds(pl.multiple_of(48 * r, 16), 48)

    mine, theirs = rows_of(rank), rows_of(z * 2 + other)
    own = [pltpu.make_async_copy(td_send.at[z, xl], synced.at[:, mine], load_sem.at[14])]
    own[0].start()
    for dz in ZAWAY:
        pltpu.make_async_remote_copy(
            td_send.at[along(dz), xl], synced.at[:, mine], a_send, a_recv, **at(along(dz), xl, g)).start()
    across = [
        pltpu.make_async_remote_copy(
            td_send.at[along(dz), other], td_relay.at[along(dz)], x_send.at[n], x_recv.at[n], **at(z, other, g))
        for n, dz in enumerate(FAR)
    ]
    for copy in across:
        copy.start()

    def waited(buf, count, sem):
        return pltpu.make_async_copy(buf.at[pl.ds(0, count)], buf.at[pl.ds(0, count)], sem)

    with jax.named_scope("wait_d"):
        waited(arr, 63, d_recv).wait()
    x = jnp.concatenate([arr[0:32].reshape(256, WIDTH), arr[32:64].reshape(256, WIDTH)], axis=1)
    r0 = lax.broadcasted_iota(jnp.int32, (256, 256), 0)
    r1 = lax.broadcasted_iota(jnp.int32, (256, 256), 1)

    def grouped(r):
        return (lax.bitwise_and(lax.shift_right_logical(r, 2), 31) * 8
                + lax.shift_right_logical(r, 7) * 4 + lax.bitwise_and(r, 3))

    order = jnp.where(grouped(r0) == r1, 1.0, 0.0).astype(BF)
    back = jnp.where(grouped(r1) == r0, 1.0, 0.0).astype(BF)
    x = dot(order, x).astype(BF)

    def push(src, dst, send_sem, recv_sem, dz):
        pltpu.make_async_remote_copy(src, dst, send_sem, recv_sem, **at(along(dz), xl, g)).start()

    def sign(c):
        return 1 if c % 2 == 0 else -1

    def partial(c):
        e = c // 2
        with jax.named_scope(f"wait_w{c}"):
            for n in range(2):
                loads[2 * c + n].wait()
                sends[2 * c + n].wait_recv()
        psend[c] = dot(x[128 * e : 128 * e + 128], wgu[c]).astype(BF).reshape(8, 16, FF)
        push(psend.at[c, along(4)], precv.at[c, 4], p_send.at[c], r_recv.at[c], 2 * sign(c))
        push(psend.at[c, along(3)], precv.at[c, 2], p_send.at[c], r_recv.at[c], 1)
        push(psend.at[c, along(-3)], precv.at[c, 3], p_send.at[c], r_recv.at[c], -1)
        push(psend.at[c, along(1)], precv.at[c, 0], p_send.at[c], p_recv.at[c], 1)
        push(psend.at[c, along(-1)], precv.at[c, 1], p_send.at[c], p_recv.at[c], -1)

    def relayed(c):
        with jax.named_scope(f"wait_r{c}"):
            waited(precv.at[c], 3, r_recv.at[c]).wait()
        ahead = psend[c, along(2)].astype(F32) + precv[c, 2].astype(F32)
        behind = psend[c, along(-2)].astype(F32) + precv[c, 3].astype(F32)
        far = precv[c, 4].astype(F32)
        if sign(c) > 0:
            ahead = ahead + far
        else:
            behind = behind + far
        pagg[c, 0] = ahead.astype(BF)
        pagg[c, 1] = behind.astype(BF)
        push(pagg.at[c, 0], precv.at[c, 5], p_send.at[c], p_recv.at[c], 2)
        push(pagg.at[c, 1], precv.at[c, 6], p_send.at[c], p_recv.at[c], -2)

    def reduced(c):
        with jax.named_scope(f"wait_p{c}"):
            waited(precv.at[c], 4, p_recv.at[c]).wait()
        total = psend[c, z].astype(F32)
        for s in (0, 1, 5, 6):
            total = total + precv[c, s].astype(F32)
        hid[c, z] = (silu(total[:, :PART]) * total[:, PART:]).astype(BF)
        block = hid.at[c, z]
        if c in DIRECT:
            for dz in ZAWAY:
                push(block, block, h_send.at[c], h_recv.at[c], dz)
        else:
            for dz in (2, -2):
                push(block, block, h_send.at[c], f_recv.at[c], dz)
            for dz in (1, -1):
                push(block, block, h_send.at[c], h_recv.at[c], dz)

    def forwarded(c):
        if c in DIRECT:
            return
        with jax.named_scope(f"wait_f{c}"):
            waited(hid.at[c], 2, f_recv.at[c]).wait()
        left, right = hid.at[c, along(-2)], hid.at[c, along(2)]
        if sign(c) > 0:
            push(left, left, h_send.at[c], h_recv.at[c], 2)
        else:
            push(right, right, h_send.at[c], h_recv.at[c], -2)
        push(left, left, h_send.at[c], h_recv.at[c], 1)
        push(right, right, h_send.at[c], h_recv.at[c], -1)

    def hop(n):
        dz = FAR[n]
        with jax.named_scope(f"wait_x{n}"):
            across[n].wait_recv()
        if dz == 0:
            own.append(pltpu.make_async_copy(td_relay.at[z], synced.at[:, theirs], load_sem.at[15]))
            own[1].start()
        else:
            push(td_relay.at[along(dz)], synced.at[:, theirs], b_send, b_recv, dz)

    stages = (partial, relayed, reduced, forwarded)
    for step in ORDER:
        stages[step // 10](step % 10)

    for n in range(EARLY):
        hop(n)
    outs = []
    for e in range(2):
        with jax.named_scope("wait_wd"):
            loads[8 + e].wait()
            sends[8 + e].wait_recv()
        out = None
        for half in range(2):
            c = 2 * e + half
            with jax.named_scope(f"wait_h{c}"):
                waited(hid.at[c], 7 if c in DIRECT else 5, h_recv.at[c]).wait()
            term = dot(hid[c].reshape(128, PART), wd[e, PART * half : PART * half + PART])
            out = term if out is None else out + term
        outs.append(out.astype(BF))
    out = dot(back, jnp.concatenate(outs, axis=0)).astype(BF)
    for n in range(2):
        oute[32 * n : 32 * n + 32] = out[:, 128 * n : 128 * n + 128].reshape(32, 8, WIDTH)
    ret[seat] = oute[xl * 32 + g]
    with jax.named_scope("issue_e"):
        for dy, flip in AWAY:
            px, pg = away(dy, flip)
            pltpu.make_async_remote_copy(
                oute.at[px * 32 + pg], ret.at[seat], e_send, e_recv, **at(z, px, pg)).start()

    for n in range(EARLY, 8):
        hop(n)
    with jax.named_scope("wait_e"):
        waited(ret, 63, e_recv).wait()
    mixed[...] = lax.dot_general(
        combine[...], ret[...].reshape(slots, WIDTH).astype(F32), (((0,), (0,)), ((), ())),
        precision=lax.Precision.HIGHEST, preferred_element_type=F32,
    ).astype(BF)

    with jax.named_scope("wait_a"):
        for copy in own:
            copy.wait()
        for sem in (a_recv, a_send, b_recv, b_send):
            waited(td_relay, 7, sem).wait()
        for copy in across:
            copy.wait_send()

    with jax.named_scope("wait_sends"):
        waited(out_tok, 63, d_send).wait()
        waited(oute, 63, e_send).wait()
        for c in range(CHUNKS):
            waited(psend.at[c], 7, p_send.at[c]).wait()
            waited(hid.at[c], 7, h_send.at[c]).wait()
        for send in sends:
            send.wait_send()


def write_out(mixed, synced, mixed_out, synced_out, sem):
    copies = [
        pltpu.make_async_copy(mixed, mixed_out, sem.at[0]),
        pltpu.make_async_copy(synced, synced_out, sem.at[1]),
    ]
    for copy in copies:
        copy.start()
    for copy in copies:
        copy.wait()


def local(tokens, routes, route_weight, gate, up, down, trained):
    V, A = pl.BlockSpec(memory_space=pltpu.VMEM), pl.BlockSpec(memory_space=pl.ANY)
    dma = pltpu.SemaphoreType.DMA
    FF = gate.shape[2]
    out = pl.pallas_call(
        kernel,
        out_shape=(pltpu.VMEM(tokens.shape, BF), pltpu.VMEM(down.shape, BF)),
        in_specs=[A] * 7,
        out_specs=(V, V),
        scratch_shapes=[
            pltpu.VMEM(tokens.shape, BF),
            pltpu.VMEM((8, 32), jnp.int32),
            pltpu.VMEM((8, 32), F32),
            pltpu.VMEM((64, 8, 128), BF),
            pltpu.VMEM((64, 8, 128), BF),
            pltpu.VMEM((CHUNKS, 256, FF), BF),
            pltpu.VMEM((2, FF, 256), BF),
            pltpu.VMEM((CHUNKS, 8, 16, FF), BF),
            pltpu.VMEM((CHUNKS, 7, 16, FF), BF),
            pltpu.VMEM((CHUNKS, 2, 16, FF), BF),
            pltpu.VMEM((CHUNKS, 8, 16, FF // 2), BF),
            pltpu.VMEM((64, 8, 128), BF),
            pltpu.VMEM((64, 8, 128), BF),
            pltpu.VMEM(trained.shape, F32),
            pltpu.VMEM((8, 2, 4, 48, 128), BF),
            pltpu.VMEM((8, 4, 48, 128), BF),
            pltpu.VMEM((512, 32), F32),
            dma((16,)), dma((10,)), dma((10,)), dma, dma, dma((CHUNKS,)), dma((CHUNKS,)),
            dma((CHUNKS,)), dma((CHUNKS,)), dma, dma, dma, dma, dma((8,)), dma((8,)), dma, dma, dma((CHUNKS,)), dma((CHUNKS,)),
        ],
        compiler_params=pltpu.CompilerParams(collective_id=0, has_side_effects=True),
        name="moe_step",
    )(tokens, routes.T, route_weight.T, gate, up, down, trained)
    out = [pltpu.with_memory_space_constraint(o, pltpu.VMEM) for o in out]
    return pl.pallas_call(
        write_out,
        out_shape=(jax.ShapeDtypeStruct(tokens.shape, BF), jax.ShapeDtypeStruct(down.shape, BF)),
        in_specs=[V, V],
        out_specs=(A, A),
        scratch_shapes=[dma((2,))],
        name="write_out",
    )(*out)


def solution(mesh):
    torus = Mesh(mesh.devices.reshape(8, 2, mesh.shape["expert"]), ("z", "xl", "expert"))
    placed = (
        P("expert", DP),
        P("expert", None),
        P("expert", None),
        P("expert", DP, None),
        P("expert", DP, None),
        P("expert", None, DP),
        P("expert", DP, None),
    )
    return jax.shard_map(
        local,
        mesh=torus,
        in_specs=placed,
        out_specs=(P("expert", DP), P("expert", None, DP)),
        check_vma=False,
    )
```

```python
import jax
import jax.numpy as jnp
from jax import lax
from jax.experimental import pallas as pl
from jax.experimental.pallas import tpu as pltpu
from jax.sharding import Mesh
from jax.sharding import PartitionSpec as P

DP = ("z", "xl")
BF = jnp.bfloat16
F32 = jnp.float32
MESH = pl.DeviceIdType.MESH
PIECES = ((640, 128, 0), (0, 384, 0), (384, 256, 0), (0, 384, 1), (384, 256, 1))
STRAIGHT = ()
DIRECT = (0, 3, 4)
EARLY = 4
SOON = 1
ORDER = (0, 1, 2, 10, 11, 3, 12, 20, 4, 21, 13, 22, 40, 14, 31, 32, 23, 30, 24, 33, 34)
AWAY = sorted(
    ((dy, flip) for dy in range(8) for flip in range(8) if dy or flip),
    key=lambda a: -(min(a[0], 8 - a[0]) + (a[1] >> 2) * 2 * (1 - (a[1] & 1)) + (a[1] & 1)),
)
ZAWAY = (4, 3, 5, 2, 6, 1, 7)
FAR = ZAWAY + (0,)


def dot(a, b, precision=None):
    return jnp.dot(a, b, preferred_element_type=F32, precision=precision)


def silu(v):
    return v / (1.0 + jnp.exp(-v))


def bits(v, shift, mask):
    return lax.bitwise_and(lax.shift_right_logical(v, shift), mask)


def experts_in(n):
    return 4 if n == 0 else 1


def kernel(*refs):
    (tokens_hbm, routes_hbm, route_weight_hbm, gate, up, down, trained, mixed, synced,
     tokens, routes, route_weight, out_tok, arr_s, arr_o, wd, oute, ret, td, td_send, td_relay, combine,
     half_sum, half_send, half_recv) = refs[:25]
    (load_sem, wl_sem, w_send, w_recv, d_send, d_recv, o_recv, p_send, p_recv, r_recv, h_send, h_recv, f_recv,
     e_send, e_recv, a_send, a_recv, b_send, b_recv, x_send, x_recv, half_sem, s_sem) = refs[25:48]
    count = len(PIECES)
    weights, leaving, psend, precv, pagg, hid = (refs[48 + count * i : 48 + count * (i + 1)] for i in range(6))

    z, xl, g = lax.axis_index("z"), lax.axis_index("xl"), lax.axis_index("expert")
    other = 1 - xl
    seat = g * 2 + xl
    rank = z * 2 + xl
    TOK, WIDTH = tokens.shape

    def at(z_, xl_, g_):
        return dict(device_id={"z": z_, "xl": xl_, "expert": g_}, device_id_type=MESH)

    def away(dy, flip):
        y = lax.bitwise_and(g + 2 * dy, 14)
        high = lax.bitwise_and(g, 16)
        high = 16 - high if flip & 4 else high
        core = lax.bitwise_and(g, 1)
        core = 1 - core if flip & 2 else core
        return (other if flip & 1 else xl), high + y + core

    def along(dz):
        return lax.bitwise_and(z + dz, 7)

    small = [
        pltpu.make_async_copy(a, b, load_sem.at[n])
        for n, (a, b) in enumerate(((routes_hbm, routes), (route_weight_hbm, route_weight), (tokens_hbm, tokens)))
    ]
    for load in small:
        load.start()

    with jax.named_scope("signals"):
        barrier = pltpu.get_barrier_semaphore()
        for dy, flip in AWAY:
            px, pg = away(dy, flip)
            pl.semaphore_signal(barrier, inc=1, **at(z, px, pg))
        for dz in ZAWAY:
            pl.semaphore_signal(barrier, inc=1, **at(along(dz), xl, g))

    load_td = pltpu.make_async_copy(trained, td, load_sem.at[3])
    load_td.start()
    loads = [[] for _ in PIECES]
    sends = [[] for _ in PIECES]
    staged = []
    for n, (first, width, e) in enumerate(PIECES):
        for m, src in enumerate((gate, up)):
            cols, into = pl.ds(first, width), pl.ds(width * m, width)
            if n == 0:
                for q in range(4):
                    pair = xl if q < 2 else other
                    loads[0].append(pltpu.make_async_copy(
                        src.at[2 * pair + q % 2, :, cols], weights[0].at[q, :, into], wl_sem.at[4 * m + q]))
            else:
                loads[n].append(pltpu.make_async_copy(
                    src.at[2 * xl + e, :, cols], weights[n].at[0:WIDTH, into], wl_sem.at[6 + 2 * n + m]))
                staged.append(pltpu.make_async_copy(
                    src.at[2 * other + e, :, cols], leaving[n].at[:, into], s_sem.at[2 * n + m]))
                sends[n].append(pltpu.make_async_remote_copy(
                    leaving[n].at[:, into], weights[n].at[WIDTH : 2 * WIDTH, into],
                    w_send.at[2 * n + m], w_recv.at[2 * n + m], **at(z, other, g)))
    down_loads, down_sends, down_staged = [], [], []
    for e in range(2):
        down_loads.append(pltpu.make_async_copy(down.at[2 * xl + e], wd.at[e, :, 0:WIDTH], load_sem.at[4 + e]))
        down_staged.append(pltpu.make_async_copy(down.at[2 * other + e], leaving[0].at[e], s_sem.at[e]))
        down_sends.append(pltpu.make_async_remote_copy(
            leaving[0].at[e], wd.at[e, :, WIDTH : 2 * WIDTH], w_send.at[e], w_recv.at[e], **at(z, other, g)))
    for load in staged + sum(loads, []) + down_staged + down_loads:
        load.start()

    with jax.named_scope("routing"):
        for load in small:
            load.wait()
        slots = 512
        row = lax.broadcasted_iota(jnp.int32, (slots, TOK), 0)
        chosen = jnp.zeros((slots, TOK), F32)
        weight = jnp.zeros((slots, TOK), F32)
        for k in range(8):
            hit = routes[k : k + 1, :] == lax.shift_right_logical(row, 2)
            chosen = jnp.where(hit, 1.0, chosen)
            weight = jnp.where(hit, route_weight[k : k + 1, :], weight)
        before = lax.broadcasted_iota(jnp.int32, (TOK, TOK), 0) < lax.broadcasted_iota(jnp.int32, (TOK, TOK), 1)
        earlier = dot(chosen.astype(BF), jnp.where(before, 1.0, 0.0).astype(BF))
        slot = lax.bitwise_and(row, 3).astype(F32)
        placed = jnp.where((chosen > 0.5) & (earlier == slot), 1.0, 0.0)
        combine[...] = placed * weight
        out_tok[...] = dot(placed.astype(BF), tokens[...]).astype(BF).reshape(64, 8, WIDTH)
        arr_s[2 * g] = out_tok[2 * g]
        arr_s[2 * g + 1] = out_tok[2 * g + 1]

    for copy in staged + down_staged:
        copy.wait()
    with jax.named_scope("barrier"):
        pl.semaphore_wait(barrier, 70)

    with jax.named_scope("issue"):
        for dy, flip in AWAY:
            px, pg = away(dy, flip)
            if flip & 1:
                pltpu.make_async_remote_copy(
                    out_tok.at[pg * 2 + px], arr_o.at[g], d_send, o_recv, **at(z, px, pg)).start()
            else:
                pltpu.make_async_remote_copy(
                    out_tok.at[pl.ds(pg * 2, 2)], arr_s.at[pl.ds(g * 2, 2)], d_send, d_recv, **at(z, px, pg)).start()
        for send in sum(sends, []) + down_sends[:SOON]:
            send.start()

    with jax.named_scope("cast"):
        load_td.wait()
        for r in range(16):
            td_send[r // 2, r % 2] = td[:, :, 128 * r : 128 * r + 128].astype(BF)

    def rows_of(r):
        return pl.ds(pl.multiple_of(48 * r, 16), 48)

    def push(src, dst, send_sem, recv_sem, dz):
        pltpu.make_async_remote_copy(src, dst, send_sem, recv_sem, **at(along(dz), xl, g)).start()

    mine, theirs = rows_of(rank), rows_of(z * 2 + other)
    own = [pltpu.make_async_copy(td_send.at[z, xl], synced.at[:, mine], load_sem.at[6])]
    own[0].start()
    for dz in ZAWAY:
        push(td_send.at[along(dz), xl], synced.at[:, mine], a_send, a_recv, dz)
    across = [
        pltpu.make_async_remote_copy(
            td_send.at[along(dz), other], td_relay.at[along(dz)], x_send.at[n], x_recv.at[n], **at(z, other, g))
        for n, dz in enumerate(FAR)
    ]

    def waited(buf, n, sem):
        return pltpu.make_async_copy(buf.at[pl.ds(0, n)], buf.at[pl.ds(0, n)], sem)

    with jax.named_scope("wait_d"):
        waited(arr_s, 62, d_recv).wait()
        waited(arr_o, 32, o_recv).wait()
    r0 = lax.broadcasted_iota(jnp.int32, (512, 512), 0)
    r1 = lax.broadcasted_iota(jnp.int32, (512, 512), 1)
    pair = lax.bitwise_and(lax.shift_right_logical(r0, 8) + xl, 1)
    source = bits(r0, 2, 31) * 16 + pair * 8 + bits(r0, 7, 1) * 4 + bits(r0, 0, 3)
    x_own = dot(jnp.where(source == r1, 1.0, 0.0).astype(BF), arr_s[...].reshape(512, WIDTH)).astype(BF)

    def grouped(r):
        return bits(r, 2, 31) * 8 + bits(r, 7, 1) * 4 + bits(r, 0, 3)

    r0, r1 = r0[:256, :256], r1[:256, :256]
    order = jnp.where(grouped(r0) == r1, 1.0, 0.0).astype(BF)
    back = jnp.where(grouped(r1) == r0, 1.0, 0.0).astype(BF)
    x_both = jnp.concatenate([x_own[:256], dot(order, arr_o[...].reshape(256, WIDTH)).astype(BF)], axis=1)

    def sign(n):
        return 1 if n % 2 == 0 else -1

    def partial(n):
        width, e = PIECES[n][1:]
        with jax.named_scope(f"wait_w{n}"):
            for copy in loads[n]:
                copy.wait()
            for copy in sends[n]:
                copy.wait_recv()
        if n == 0:
            for q in range(4):
                psend[0][:, q] = dot(x_own[128 * q : 128 * q + 128], weights[0][q]).astype(BF).reshape(8, 16, 2 * width)
        else:
            psend[n][:, 0] = dot(x_both[128 * e : 128 * e + 128], weights[n][...]).astype(BF).reshape(8, 16, 2 * width)
        if n in STRAIGHT:
            for m, dz in enumerate(ZAWAY):
                push(psend[n].at[along(dz)], precv[n].at[m], p_send.at[n], p_recv.at[n], dz)
            return
        push(psend[n].at[along(4)], precv[n].at[4], p_send.at[n], r_recv.at[n], 2 * sign(n))
        push(psend[n].at[along(3)], precv[n].at[2], p_send.at[n], r_recv.at[n], 1)
        push(psend[n].at[along(-3)], precv[n].at[3], p_send.at[n], r_recv.at[n], -1)
        push(psend[n].at[along(1)], precv[n].at[0], p_send.at[n], p_recv.at[n], 1)
        push(psend[n].at[along(-1)], precv[n].at[1], p_send.at[n], p_recv.at[n], -1)

    def relayed(n):
        if n in STRAIGHT:
            return
        with jax.named_scope(f"wait_r{n}"):
            waited(precv[n], 3, r_recv.at[n]).wait()
        ahead = psend[n][along(2)].astype(F32) + precv[n][2].astype(F32)
        behind = psend[n][along(-2)].astype(F32) + precv[n][3].astype(F32)
        far = precv[n][4].astype(F32)
        if sign(n) > 0:
            ahead = ahead + far
        else:
            behind = behind + far
        pagg[n][0] = ahead.astype(BF)
        pagg[n][1] = behind.astype(BF)
        push(pagg[n].at[0], precv[n].at[5], p_send.at[n], p_recv.at[n], 2)
        push(pagg[n].at[1], precv[n].at[6], p_send.at[n], p_recv.at[n], -2)

    def activated(n, total):
        width = PIECES[n][1]
        hid[n][z] = (silu(total[:, :, :width]) * total[:, :, width:]).astype(BF)
        block = hid[n].at[z]
        if n in DIRECT:
            for dz in ZAWAY:
                push(block, block, h_send.at[n], h_recv.at[n], dz)
        else:
            for dz in (2, -2):
                push(block, block, h_send.at[n], f_recv.at[n], dz)
            for dz in (1, -1):
                push(block, block, h_send.at[n], h_recv.at[n], dz)

    halves = pltpu.make_async_remote_copy(half_send, half_recv, half_sem.at[0], half_sem.at[1], **at(z, other, g))

    def reduced(n):
        with jax.named_scope(f"wait_p{n}"):
            waited(precv[n], 7 if n in STRAIGHT else 4, p_recv.at[n]).wait()
        total = psend[n][z].astype(F32)
        for s in range(7) if n in STRAIGHT else (0, 1, 5, 6):
            total = total + precv[n][s].astype(F32)
        if n == 0:
            half_send[...] = total[2:].astype(BF)
            half_sum[...] = total[:2]
            halves.start()
            for copy in down_sends[SOON:] + across:
                copy.start()
        else:
            activated(n, total)

    def both_halves(n):
        with jax.named_scope("wait_half"):
            halves.wait_recv()
        activated(n, half_sum[...] + half_recv[...].astype(F32))

    def forwarded(n):
        if n in DIRECT:
            return
        with jax.named_scope(f"wait_f{n}"):
            waited(hid[n], 2, f_recv.at[n]).wait()
        left, right = hid[n].at[along(-2)], hid[n].at[along(2)]
        if sign(n) > 0:
            push(left, left, h_send.at[n], h_recv.at[n], 2)
        else:
            push(right, right, h_send.at[n], h_recv.at[n], -2)
        push(left, left, h_send.at[n], h_recv.at[n], 1)
        push(right, right, h_send.at[n], h_recv.at[n], -1)

    def hop(n):
        dz = FAR[n]
        with jax.named_scope(f"wait_x{n}"):
            across[n].wait_recv()
        if dz == 0:
            own.append(pltpu.make_async_copy(td_relay.at[z], synced.at[:, theirs], load_sem.at[7]))
            own[1].start()
        else:
            push(td_relay.at[along(dz)], synced.at[:, theirs], b_send, b_recv, dz)

    stages = (partial, relayed, reduced, forwarded, both_halves)
    for step in ORDER:
        stages[step // 10](step % 10)

    for n in range(EARLY):
        hop(n)
    with jax.named_scope("wait_wd"):
        for e in range(2):
            down_loads[e].wait()
            down_sends[e].wait_recv()
    outs = [None, None]
    for n, (first, width, expert) in enumerate(PIECES):
        with jax.named_scope(f"wait_h{n}"):
            waited(hid[n], 7 if n in DIRECT else 5, h_recv.at[n]).wait()
        for m, e in enumerate((0, 1) if n == 0 else (expert,)):
            term = dot(hid[n][:, m].reshape(128, width), wd[e, first : first + width])
            outs[e] = term if outs[e] is None else outs[e] + term
    out = dot(back, jnp.concatenate(outs, axis=0).astype(BF)).astype(BF)
    for n in range(2):
        oute[32 * n : 32 * n + 32] = out[:, WIDTH * n : WIDTH * n + WIDTH].reshape(32, 8, WIDTH)
    ret[seat] = oute[g]
    with jax.named_scope("issue_e"):
        for dy, flip in AWAY:
            px, pg = away(dy, flip)
            pltpu.make_async_remote_copy(
                oute.at[(flip & 1) * 32 + pg], ret.at[seat], e_send, e_recv, **at(z, px, pg)).start()

    for n in range(EARLY, 8):
        hop(n)
    with jax.named_scope("wait_e"):
        waited(ret, 63, e_recv).wait()
    mixed[...] = lax.dot_general(
        combine[...], ret[...].reshape(slots, WIDTH).astype(F32), (((0,), (0,)), ((), ())),
        precision=lax.Precision.HIGHEST, preferred_element_type=F32,
    ).astype(BF)

    with jax.named_scope("wait_a"):
        for copy in own:
            copy.wait()
        for sem in (a_recv, a_send, b_recv, b_send):
            waited(td_relay, 7, sem).wait()
        for copy in across:
            copy.wait_send()
    with jax.named_scope("wait_sends"):
        waited(out_tok, 62, d_send).wait()
        waited(out_tok, 32, d_send).wait()
        waited(oute, 63, e_send).wait()
        halves.wait_send()
        for n in range(count):
            waited(psend[n], 7, p_send.at[n]).wait()
            waited(hid[n], 7, h_send.at[n]).wait()
        for send in sum(sends, []) + down_sends:
            send.wait_send()


def write_out(mixed, synced, mixed_out, synced_out, sem):
    copies = [
        pltpu.make_async_copy(synced, synced_out, sem.at[1]),
        pltpu.make_async_copy(mixed, mixed_out, sem.at[0]),
    ]
    for copy in copies:
        copy.start()
    for copy in copies:
        copy.wait()


def local(tokens, routes, route_weight, gate, up, down, trained):
    V, A = pl.BlockSpec(memory_space=pltpu.VMEM), pl.BlockSpec(memory_space=pl.ANY)
    FF = gate.shape[2]
    count = len(PIECES)
    wide = [2 * width for _, width, _ in PIECES]

    def vmem(*shape, dtype=BF):
        return pltpu.VMEM(shape, dtype)

    def dma(*shape):
        return pltpu.SemaphoreType.DMA(shape)

    scratch = [
        vmem(*tokens.shape), vmem(8, 32, dtype=jnp.int32), vmem(8, 32, dtype=F32),
        vmem(64, 8, 128), vmem(64, 8, 128), vmem(32, 8, 128), vmem(2, FF, 256), vmem(64, 8, 128), vmem(64, 8, 128),
        vmem(*trained.shape, dtype=F32), vmem(8, 2, 4, 48, 128), vmem(8, 4, 48, 128), vmem(512, 32, dtype=F32),
        vmem(2, 16, wide[0], dtype=F32), vmem(2, 16, wide[0]), vmem(2, 16, wide[0]),
        dma(8), dma(8 + 2 * count), dma(2 * count), dma(2 * count), dma(), dma(), dma(),
        dma(count), dma(count), dma(count), dma(count), dma(count), dma(count),
        dma(), dma(), dma(), dma(), dma(), dma(), dma(8), dma(8), dma(2), dma(2 * count),
    ]
    scratch += [vmem(*((4, 128, wide[0]) if n == 0 else (256, wide[n]))) for n in range(count)]
    scratch += [vmem(*((2, FF, 128) if n == 0 else (128, wide[n]))) for n in range(count)]
    for devices in (8, 7, 2):
        scratch += [vmem(devices, experts_in(n), 16, wide[n]) for n in range(count)]
    scratch += [vmem(8, 2 if n == 0 else 1, 16, wide[n] // 2) for n in range(count)]
    out = pl.pallas_call(
        kernel,
        out_shape=(pltpu.VMEM(tokens.shape, BF), pltpu.VMEM(down.shape, BF)),
        in_specs=[A] * 7,
        out_specs=(V, V),
        scratch_shapes=scratch,
        compiler_params=pltpu.CompilerParams(collective_id=0, has_side_effects=True),
        name="moe_step",
    )(tokens, routes.T, route_weight.T, gate, up, down, trained)
    out = [pltpu.with_memory_space_constraint(o, pltpu.VMEM) for o in out]
    return pl.pallas_call(
        write_out,
        out_shape=(jax.ShapeDtypeStruct(tokens.shape, BF), jax.ShapeDtypeStruct(down.shape, BF)),
        in_specs=[V, V],
        out_specs=(A, A),
        scratch_shapes=[dma(2)],
        name="write_out",
    )(*out)


def solution(mesh):
    torus = Mesh(mesh.devices.reshape(8, 2, mesh.shape["expert"]), ("z", "xl", "expert"))
    placed = (
        P("expert", DP),
        P("expert", None),
        P("expert", None),
        P("expert", DP, None),
        P("expert", DP, None),
        P("expert", None, DP),
        P("expert", DP, None),
    )
    return jax.shard_map(
        local,
        mesh=torus,
        in_specs=placed,
        out_specs=(P("expert", DP), P("expert", None, DP)),
        check_vma=False,
    )
```

```python
import jax
import jax.numpy as jnp
from jax import lax
from jax.experimental import pallas as pl
from jax.experimental.pallas import tpu as pltpu
from jax.sharding import Mesh
from jax.sharding import PartitionSpec as P

DP = ("z", "xl")
BF = jnp.bfloat16
F32 = jnp.float32
MESH = pl.DeviceIdType.MESH
PIECES = ((640, 128, 0), (0, 384, 0), (384, 256, 0), (0, 384, 1), (384, 256, 1))
STRAIGHT = ()
DIRECT = (3, 4)
EARLY = 2
SOON = 1
ORDER = (0, 1, 2, 10, 11, 3, 12, 20, 4, 21, 13, 22, 40, 14, 31, 32, 23, 30, 24, 33, 34)
AWAY = sorted(
    ((dy, flip) for dy in range(8) for flip in range(8) if dy or flip),
    key=lambda a: -(min(a[0], 8 - a[0]) + (a[1] >> 2) * 2 * (1 - (a[1] & 1)) + (a[1] & 1)),
)
ZAWAY = (4, 3, 5, 2, 6, 1, 7)
FAR = ZAWAY + (0,)


def dot(a, b, precision=None):
    return jnp.dot(a, b, preferred_element_type=F32, precision=precision)


def silu(v):
    return v / (1.0 + jnp.exp(-v))


def bits(v, shift, mask):
    return lax.bitwise_and(lax.shift_right_logical(v, shift), mask)


def experts_in(n):
    return 4 if n == 0 else 1


def kernel(*refs):
    (tokens_hbm, routes_hbm, route_weight_hbm, gate, up, down, trained, ret, shares, synced,
     tokens, routes, route_weight, out_tok, arr_s, arr_o, wd, oute, td, td_send, td_relay, td_far, combine,
     half_sum, half_send, half_recv) = refs[:26]
    (load_sem, wl_sem, sent, w_recv, d_recv, o_recv, p_recv, r_recv, h_recv, f_recv,
     e_recv, a_recv, b_recv, x_recv, half_sem, s_sem, v_recv) = refs[26:43]
    count = len(PIECES)
    weights, leaving, psend, precv, pagg, hid = (refs[43 + count * i : 43 + count * (i + 1)] for i in range(6))

    z, xl, g = lax.axis_index("z"), lax.axis_index("xl"), lax.axis_index("expert")
    other = 1 - xl
    seat = g * 2 + xl
    rank = z * 2 + xl
    core = lax.bitwise_and(g, 1)
    TOK, WIDTH = tokens.shape

    def at(z_, xl_, g_):
        return dict(device_id={"z": z_, "xl": xl_, "expert": g_}, device_id_type=MESH)

    def away(dy, flip):
        y = lax.bitwise_and(g + 2 * dy, 14)
        high = lax.bitwise_and(g, 16)
        high = 16 - high if flip & 4 else high
        side = 1 - core if flip & 2 else core
        return (other if flip & 1 else xl), high + y + side

    def along(dz):
        return lax.bitwise_and(z + dz, 7)

    small = [
        pltpu.make_async_copy(a, b, load_sem.at[n])
        for n, (a, b) in enumerate(((routes_hbm, routes), (route_weight_hbm, route_weight), (tokens_hbm, tokens)))
    ]
    for load in small:
        load.start()

    with jax.named_scope("signals"):
        barrier = pltpu.get_barrier_semaphore()
        for dy, flip in AWAY:
            px, pg = away(dy, flip)
            pl.semaphore_signal(barrier, inc=1, **at(z, px, pg))
        for dz in ZAWAY:
            pl.semaphore_signal(barrier, inc=1, **at(along(dz), xl, g))

    load_td = pltpu.make_async_copy(trained, td, load_sem.at[3])
    load_td.start()
    loads = [[] for _ in PIECES]
    sends = [[] for _ in PIECES]
    staged = []
    for n, (first, width, e) in enumerate(PIECES):
        for m, src in enumerate((gate, up)):
            cols, into = pl.ds(first, width), pl.ds(width * m, width)
            if n == 0:
                for q in range(4):
                    pair = xl if q < 2 else other
                    loads[0].append(pltpu.make_async_copy(
                        src.at[2 * pair + q % 2, :, cols], weights[0].at[q, :, into], wl_sem.at[4 * m + q]))
            else:
                loads[n].append(pltpu.make_async_copy(
                    src.at[2 * xl + e, :, cols], weights[n].at[0:WIDTH, into], wl_sem.at[6 + 2 * n + m]))
                staged.append(pltpu.make_async_copy(
                    src.at[2 * other + e, :, cols], leaving[n].at[:, into], s_sem))
                sends[n].append(pltpu.make_async_remote_copy(
                    leaving[n].at[:, into], weights[n].at[WIDTH : 2 * WIDTH, into],
                    sent, w_recv.at[2 * n + m], **at(z, other, g)))
    down_loads, down_sends, down_staged = [], [], []
    for e in range(2):
        down_loads.append(pltpu.make_async_copy(down.at[2 * xl + e], wd.at[e, :, 0:WIDTH], load_sem.at[4 + e]))
        down_staged.append(pltpu.make_async_copy(down.at[2 * other + e], leaving[0].at[e], s_sem))
        down_sends.append(pltpu.make_async_remote_copy(
            leaving[0].at[e], wd.at[e, :, WIDTH : 2 * WIDTH], sent, w_recv.at[e], **at(z, other, g)))
    for load in staged + sum(loads, []) + down_staged + down_loads:
        load.start()

    with jax.named_scope("routing"):
        for load in small:
            load.wait()
        slots = 512
        row = lax.broadcasted_iota(jnp.int32, (slots, TOK), 0)
        chosen = jnp.zeros((slots, TOK), F32)
        weight = jnp.zeros((slots, TOK), F32)
        for k in range(8):
            hit = routes[k : k + 1, :] == lax.shift_right_logical(row, 2)
            chosen = jnp.where(hit, 1.0, chosen)
            weight = jnp.where(hit, route_weight[k : k + 1, :], weight)
        before = lax.broadcasted_iota(jnp.int32, (TOK, TOK), 0) < lax.broadcasted_iota(jnp.int32, (TOK, TOK), 1)
        earlier = dot(chosen.astype(BF), jnp.where(before, 1.0, 0.0).astype(BF))
        slot = lax.bitwise_and(row, 3).astype(F32)
        placed = jnp.where((chosen > 0.5) & (earlier == slot), 1.0, 0.0)
        combine[...] = placed * weight
        out_tok[...] = dot(placed.astype(BF), tokens[...]).astype(BF).reshape(64, 8, WIDTH)
        arr_s[2 * g] = out_tok[2 * g]
        arr_s[2 * g + 1] = out_tok[2 * g + 1]

    for copy in staged + down_staged:
        copy.wait()
    with jax.named_scope("barrier"):
        pl.semaphore_wait(barrier, 70)

    with jax.named_scope("issue"):
        for dy, flip in AWAY:
            px, pg = away(dy, flip)
            if flip & 1:
                pltpu.make_async_remote_copy(
                    out_tok.at[pg * 2 + px], arr_o.at[g], sent, o_recv, **at(z, px, pg)).start()
            else:
                pltpu.make_async_remote_copy(
                    out_tok.at[pl.ds(pg * 2, 2)], arr_s.at[pl.ds(g * 2, 2)], sent, d_recv, **at(z, px, pg)).start()
        for send in sum(sends, []) + down_sends[:SOON]:
            send.start()

    with jax.named_scope("cast"):
        load_td.wait()
        for r in range(16):
            td_send[r // 2, r % 2] = td[:, :, 128 * r : 128 * r + 128].astype(BF)

    def rows_of(r):
        return pl.ds(pl.multiple_of(48 * r, 16), 48)

    def push(src, dst, send_sem, recv_sem, dz):
        pltpu.make_async_remote_copy(src, dst, send_sem, recv_sem, **at(along(dz), xl, g)).start()

    mine, theirs = rows_of(rank), rows_of(z * 2 + other)
    own = [
        pltpu.make_async_copy(td_send.at[z, xl], synced.at[:, mine], load_sem.at[6]),
        pltpu.make_async_copy(combine, shares, load_sem.at[8]),
    ]
    for copy in own:
        copy.start()

    def spread(block, rows, far, send_sem, recv_sem, dz):
        if dz == 4:
            for way in range(2):
                push(block.at[pl.ds(2 * way, 2)], td_far.at[far, way], send_sem, v_recv.at[far], 2 - 4 * way)
        else:
            push(block, synced.at[:, rows], send_sem, recv_sem, dz)

    def passed_on(far, side, send_sem, recv_sem):
        with jax.named_scope(f"wait_v{far}"):
            waited(td_far.at[far], 2, v_recv.at[far]).wait()
        for way in range(2):
            dz = 2 - 4 * way
            push(td_far.at[far, way], synced.at[pl.ds(2 * way, 2), rows_of(along(-dz) * 2 + side)], send_sem, recv_sem, dz)

    for dz in ZAWAY:
        spread(td_send.at[along(dz), xl], mine, 0, sent, a_recv, dz)
    across = [
        pltpu.make_async_remote_copy(
            td_send.at[along(dz), other], td_relay.at[along(dz)], sent, x_recv.at[n], **at(z, other, g))
        for n, dz in enumerate(FAR)
    ]

    def waited(buf, n, sem):
        return pltpu.make_async_copy(buf.at[pl.ds(0, n)], buf.at[pl.ds(0, n)], sem)

    passed_on(0, xl, sent, a_recv)
    with jax.named_scope("wait_d"):
        waited(arr_s, 62, d_recv).wait()
        waited(arr_o, 32, o_recv).wait()
    r0 = lax.broadcasted_iota(jnp.int32, (512, 512), 0)
    r1 = lax.broadcasted_iota(jnp.int32, (512, 512), 1)
    pair = lax.bitwise_and(lax.shift_right_logical(r0, 8) + xl, 1)
    source = bits(r0, 2, 31) * 16 + pair * 8 + bits(r0, 7, 1) * 4 + bits(r0, 0, 3)
    x_own = dot(jnp.where(source == r1, 1.0, 0.0).astype(BF), arr_s[...].reshape(512, WIDTH)).astype(BF)

    def grouped(r):
        return bits(r, 2, 31) * 8 + bits(r, 7, 1) * 4 + bits(r, 0, 3)

    r0, r1 = r0[:256, :256], r1[:256, :256]
    order = jnp.where(grouped(r0) == r1, 1.0, 0.0).astype(BF)
    back = jnp.where(grouped(r1) == r0, 1.0, 0.0).astype(BF)
    x_both = jnp.concatenate([x_own[:256], dot(order, arr_o[...].reshape(256, WIDTH)).astype(BF)], axis=1)

    def sign(n):
        return 1 if n % 2 == 0 else -1

    def partial(n):
        width, e = PIECES[n][1:]
        with jax.named_scope(f"wait_w{n}"):
            for copy in loads[n]:
                copy.wait()
            for copy in sends[n]:
                copy.wait_recv()
        if n == 0:
            for q in range(4):
                psend[0][:, q] = dot(x_own[128 * q : 128 * q + 128], weights[0][q]).astype(BF).reshape(8, 16, 2 * width)
        else:
            psend[n][:, 0] = dot(x_both[128 * e : 128 * e + 128], weights[n][...]).astype(BF).reshape(8, 16, 2 * width)
        if n in STRAIGHT:
            for m, dz in enumerate(ZAWAY):
                push(psend[n].at[along(dz)], precv[n].at[m], sent, p_recv.at[n], dz)
            return
        push(psend[n].at[along(4)], precv[n].at[4], sent, r_recv.at[n], 2 * sign(n))
        push(psend[n].at[along(3)], precv[n].at[2], sent, r_recv.at[n], 1)
        push(psend[n].at[along(-3)], precv[n].at[3], sent, r_recv.at[n], -1)
        push(psend[n].at[along(1)], precv[n].at[0], sent, p_recv.at[n], 1)
        push(psend[n].at[along(-1)], precv[n].at[1], sent, p_recv.at[n], -1)

    def relayed(n):
        if n in STRAIGHT:
            return
        with jax.named_scope(f"wait_r{n}"):
            waited(precv[n], 3, r_recv.at[n]).wait()
        ahead = psend[n][along(2)].astype(F32) + precv[n][2].astype(F32)
        behind = psend[n][along(-2)].astype(F32) + precv[n][3].astype(F32)
        far = precv[n][4].astype(F32)
        if sign(n) > 0:
            ahead = ahead + far
        else:
            behind = behind + far
        pagg[n][0] = ahead.astype(BF)
        pagg[n][1] = behind.astype(BF)
        push(pagg[n].at[0], precv[n].at[5], sent, p_recv.at[n], 2)
        push(pagg[n].at[1], precv[n].at[6], sent, p_recv.at[n], -2)

    def activated(n, total):
        width = PIECES[n][1]
        hid[n][z] = (silu(total[:, :, :width]) * total[:, :, width:]).astype(BF)
        block = hid[n].at[z]
        if n in DIRECT:
            for dz in ZAWAY:
                push(block, block, sent, h_recv.at[n], dz)
        else:
            for dz in (2, -2):
                push(block, block, sent, f_recv.at[n], dz)
            for dz in (1, -1):
                push(block, block, sent, h_recv.at[n], dz)

    halves = pltpu.make_async_remote_copy(half_send, half_recv, sent, half_sem, **at(z, other, g))

    def reduced(n):
        with jax.named_scope(f"wait_p{n}"):
            waited(precv[n], 7 if n in STRAIGHT else 4, p_recv.at[n]).wait()
        total = psend[n][z].astype(F32)
        for s in range(7) if n in STRAIGHT else (0, 1, 5, 6):
            total = total + precv[n][s].astype(F32)
        if n == 0:
            half_send[...] = total[2:].astype(BF)
            half_sum[...] = total[:2]
            halves.start()
            for copy in down_sends[SOON:] + across:
                copy.start()
        else:
            activated(n, total)

    def both_halves(n):
        with jax.named_scope("wait_half"):
            halves.wait_recv()
        activated(n, half_sum[...] + half_recv[...].astype(F32))

    def forwarded(n):
        if n in DIRECT:
            return
        with jax.named_scope(f"wait_f{n}"):
            waited(hid[n], 2, f_recv.at[n]).wait()
        left, right = hid[n].at[along(-2)], hid[n].at[along(2)]
        if sign(n) > 0:
            push(left, left, sent, h_recv.at[n], 2)
        else:
            push(right, right, sent, h_recv.at[n], -2)
        push(left, left, sent, h_recv.at[n], 1)
        push(right, right, sent, h_recv.at[n], -1)

    def hop(n):
        dz = FAR[n]
        with jax.named_scope(f"wait_x{n}"):
            across[n].wait_recv()
        if dz == 0:
            own.append(pltpu.make_async_copy(td_relay.at[z], synced.at[:, theirs], load_sem.at[7]))
            own[-1].start()
        else:
            spread(td_relay.at[along(dz)], theirs, 1, sent, b_recv, dz)

    stages = (partial, relayed, reduced, forwarded, both_halves)
    for step in ORDER:
        stages[step // 10](step % 10)

    for n in range(EARLY):
        hop(n)
    with jax.named_scope("wait_wd"):
        for e in range(2):
            down_loads[e].wait()
            down_sends[e].wait_recv()
    outs = [None, None]
    for n, (first, width, expert) in enumerate(PIECES):
        with jax.named_scope(f"wait_h{n}"):
            waited(hid[n], 7 if n in DIRECT else 5, h_recv.at[n]).wait()
        for m, e in enumerate((0, 1) if n == 0 else (expert,)):
            term = dot(hid[n][:, m].reshape(128, width), wd[e, first : first + width])
            outs[e] = term if outs[e] is None else outs[e] + term
    out = dot(back, jnp.concatenate(outs, axis=0).astype(BF)).astype(BF)
    for n in range(2):
        oute[32 * n : 32 * n + 32] = out[:, WIDTH * n : WIDTH * n + WIDTH].reshape(32, 8, WIDTH)
    own.append(pltpu.make_async_copy(oute.at[g], ret.at[seat], load_sem.at[9]))
    own[-1].start()
    with jax.named_scope("issue_e"):
        for dy, flip in AWAY:
            px, pg = away(dy, flip)
            pltpu.make_async_remote_copy(
                oute.at[(flip & 1) * 32 + pg], ret.at[seat], sent, e_recv, **at(z, px, pg)).start()

    for n in range(EARLY, 8):
        hop(n)
    passed_on(1, other, sent, b_recv)
    with jax.named_scope("wait_e"):
        waited(oute, 63, e_recv).wait()

    with jax.named_scope("wait_a"):
        for copy in own:
            copy.wait()
        for sem in (a_recv, b_recv):
            waited(td_relay, 7, sem).wait()
        for sem in (sent, sent):
            waited(td_relay, 8, sem).wait()
        for copy in across:
            copy.wait_send()
    with jax.named_scope("wait_sends"):
        waited(out_tok, 62, sent).wait()
        waited(out_tok, 32, sent).wait()
        waited(oute, 63, sent).wait()
        halves.wait_send()
        for n in range(count):
            waited(psend[n], 7, sent).wait()
            waited(hid[n], 7, sent).wait()
        for send in sum(sends, []) + down_sends:
            send.wait_send()


def write_out(ret, shares, synced, mixed_out, synced_out, mixed, sem):
    copy = pltpu.make_async_copy(synced, synced_out, sem.at[1])
    copy.start()
    mixed[...] = lax.dot_general(
        shares[...], ret[...].reshape(shares.shape[0], ret.shape[2]).astype(F32), (((0,), (0,)), ((), ())),
        precision=lax.Precision.HIGHEST, preferred_element_type=F32,
    ).astype(BF)
    last = pltpu.make_async_copy(mixed, mixed_out, sem.at[0])
    last.start()
    copy.wait()
    last.wait()


def local(tokens, routes, route_weight, gate, up, down, trained):
    V, A = pl.BlockSpec(memory_space=pltpu.VMEM), pl.BlockSpec(memory_space=pl.ANY)
    FF = gate.shape[2]
    count = len(PIECES)
    wide = [2 * width for _, width, _ in PIECES]

    def vmem(*shape, dtype=BF):
        return pltpu.VMEM(shape, dtype)

    def dma(*shape):
        return pltpu.SemaphoreType.DMA(shape)

    scratch = [
        vmem(*tokens.shape), vmem(8, 32, dtype=jnp.int32), vmem(8, 32, dtype=F32),
        vmem(64, 8, 128), vmem(64, 8, 128), vmem(32, 8, 128), vmem(2, FF, 256), vmem(64, 8, 128),
        vmem(*trained.shape, dtype=F32), vmem(8, 2, 4, 48, 128), vmem(8, 4, 48, 128), vmem(2, 2, 2, 48, 128), vmem(512, 32, dtype=F32),
        vmem(2, 16, wide[0], dtype=F32), vmem(2, 16, wide[0]), vmem(2, 16, wide[0]),
        dma(10), dma(8 + 2 * count), dma(), dma(2 * count), dma(), dma(),
        dma(count), dma(count), dma(count), dma(count),
        dma(), dma(), dma(), dma(8), dma(), dma(), dma(2),
    ]
    scratch += [vmem(*((4, 128, wide[0]) if n == 0 else (256, wide[n]))) for n in range(count)]
    scratch += [vmem(*((2, FF, 128) if n == 0 else (128, wide[n]))) for n in range(count)]
    for devices in (8, 7, 2):
        scratch += [vmem(devices, experts_in(n), 16, wide[n]) for n in range(count)]
    scratch += [vmem(8, 2 if n == 0 else 1, 16, wide[n] // 2) for n in range(count)]
    out = pl.pallas_call(
        kernel,
        out_shape=(pltpu.VMEM((64, 8, 128), BF), pltpu.VMEM((512, 32), F32), pltpu.VMEM(down.shape, BF)),
        in_specs=[A] * 7,
        out_specs=(A, A, A),
        scratch_shapes=scratch,
        compiler_params=pltpu.CompilerParams(collective_id=0, has_side_effects=True),
        name="moe_step",
    )(tokens, routes.T, route_weight.T, gate, up, down, trained)
    out = [pltpu.with_memory_space_constraint(o, pltpu.VMEM) for o in out]
    return pl.pallas_call(
        write_out,
        out_shape=(jax.ShapeDtypeStruct(tokens.shape, BF), jax.ShapeDtypeStruct(down.shape, BF)),
        in_specs=[V, V, V],
        out_specs=(A, A),
        scratch_shapes=[vmem(*tokens.shape), dma(2)],
        name="write_out",
    )(*out)


def solution(mesh):
    torus = Mesh(mesh.devices.reshape(8, 2, mesh.shape["expert"]), ("z", "xl", "expert"))
    placed = (
        P("expert", DP),
        P("expert", None),
        P("expert", None),
        P("expert", DP, None),
        P("expert", DP, None),
        P("expert", None, DP),
        P("expert", DP, None),
    )
    return jax.shard_map(
        local,
        mesh=torus,
        in_specs=placed,
        out_specs=(P("expert", DP), P("expert", None, DP)),
        check_vma=False,
    )
```

```python
import jax
import jax.numpy as jnp
from jax import lax
from jax.experimental import pallas as pl
from jax.experimental.pallas import tpu as pltpu
from jax.sharding import Mesh
from jax.sharding import PartitionSpec as P

DP = ("z", "xl")
BF = jnp.bfloat16
F32 = jnp.float32
MESH = pl.DeviceIdType.MESH
PIECES = ((640, 128, 0), (0, 384, 0), (384, 256, 0), (0, 384, 1), (384, 256, 1))
STRAIGHT = ()
DIRECT = (3, 4)
EARLY = 2
SOON = 1
ORDER = (0, 1, 2, 10, 11, 3, 12, 20, 4, 21, 13, 22, 40, 14, 31, 23, 32, 30, 24, 33, 34)
AWAY = sorted(
    ((dy, flip) for dy in range(8) for flip in range(8) if dy or flip),
    key=lambda a: -(min(a[0], 8 - a[0]) + (a[1] >> 2) * 2 * (1 - (a[1] & 1)) + (a[1] & 1)),
)
ZAWAY = (4, 3, 5, 2, 6, 1, 7)
FAR = ZAWAY + (0,)


def dot(a, b, precision=None):
    return jnp.dot(a, b, preferred_element_type=F32, precision=precision)


def silu(v):
    return v / (1.0 + jnp.exp(-v))


def bits(v, shift, mask):
    return lax.bitwise_and(lax.shift_right_logical(v, shift), mask)


def experts_in(n):
    return 4 if n == 0 else 1


def kernel(*refs):
    (tokens_hbm, routes_hbm, route_weight_hbm, gate, up, down, trained, ret, shares, synced,
     tokens, routes, route_weight, out_tok, arr_s, arr_o, wd, oute, td, td_send, td_relay, td_far, combine,
     half_sum, half_send, half_recv) = refs[:26]
    (load_sem, sent, w_recv, d_recv, o_recv, p_recv, r_recv, h_recv, f_recv,
     e_recv, a_recv, b_recv, x_recv, half_sem, s_sem, v_recv) = refs[26:42]
    count = len(PIECES)
    weights, leaving, psend, precv, pagg, hid = (refs[42 + count * i : 42 + count * (i + 1)] for i in range(6))

    z, xl, g = lax.axis_index("z"), lax.axis_index("xl"), lax.axis_index("expert")
    other = 1 - xl
    seat = g * 2 + xl
    rank = z * 2 + xl
    core = lax.bitwise_and(g, 1)
    TOK, WIDTH = tokens.shape

    def at(z_, xl_, g_):
        return dict(device_id={"z": z_, "xl": xl_, "expert": g_}, device_id_type=MESH)

    def away(dy, flip):
        y = lax.bitwise_and(g + 2 * dy, 14)
        high = lax.bitwise_and(g, 16)
        high = 16 - high if flip & 4 else high
        side = 1 - core if flip & 2 else core
        return (other if flip & 1 else xl), high + y + side

    def along(dz):
        return lax.bitwise_and(z + dz, 7)

    small = [
        pltpu.make_async_copy(a, b, load_sem.at[n])
        for n, (a, b) in enumerate(((routes_hbm, routes), (route_weight_hbm, route_weight), (tokens_hbm, tokens)))
    ]
    for load in small:
        load.start()

    with jax.named_scope("signals"):
        barrier = pltpu.get_barrier_semaphore()
        for dy, flip in AWAY:
            px, pg = away(dy, flip)
            pl.semaphore_signal(barrier, inc=1, **at(z, px, pg))
        for dz in ZAWAY:
            pl.semaphore_signal(barrier, inc=1, **at(along(dz), xl, g))

    load_td = pltpu.make_async_copy(trained, td, load_sem.at[3])
    load_td.start()
    loads = [[] for _ in PIECES]
    sends = [[] for _ in PIECES]
    staged = []
    for n, (first, width, e) in enumerate(PIECES):
        for m, src in enumerate((gate, up)):
            cols, into = pl.ds(first, width), pl.ds(width * m, width)
            if n == 0:
                for q in range(4):
                    pair = xl if q < 2 else other
                    loads[0].append(pltpu.make_async_copy(
                        src.at[2 * pair + q % 2, :, cols], weights[0].at[q, :, into], s_sem))
            else:
                loads[n].append(pltpu.make_async_copy(
                    src.at[2 * xl + e, :, cols], weights[n].at[0:WIDTH, into], s_sem))
                staged.append(pltpu.make_async_copy(
                    src.at[2 * other + e, :, cols], leaving[n].at[:, into], s_sem))
        if n:
            sends[n].append(pltpu.make_async_remote_copy(
                leaving[n], weights[n].at[WIDTH : 2 * WIDTH], sent, w_recv.at[n + 1], **at(z, other, g)))
    down_loads, down_sends, down_staged = [], [], []
    for e in range(2):
        down_loads.append(pltpu.make_async_copy(down.at[2 * xl + e], wd.at[e, :, 0:WIDTH], s_sem))
        down_staged.append(pltpu.make_async_copy(down.at[2 * other + e], leaving[0].at[e], s_sem))
        down_sends.append(pltpu.make_async_remote_copy(
            leaving[0].at[e], wd.at[e, :, WIDTH : 2 * WIDTH], sent, w_recv.at[e], **at(z, other, g)))
    for load in staged + sum(loads, []) + down_staged + down_loads:
        load.start()

    with jax.named_scope("routing"):
        for load in small:
            load.wait()
        slots = 512
        row = lax.broadcasted_iota(jnp.int32, (slots, TOK), 0)
        chosen = jnp.zeros((slots, TOK), F32)
        weight = jnp.zeros((slots, TOK), F32)
        for k in range(8):
            hit = routes[k : k + 1, :] == lax.shift_right_logical(row, 2)
            chosen = jnp.where(hit, 1.0, chosen)
            weight = jnp.where(hit, route_weight[k : k + 1, :], weight)
        before = lax.broadcasted_iota(jnp.int32, (TOK, TOK), 0) < lax.broadcasted_iota(jnp.int32, (TOK, TOK), 1)
        earlier = dot(chosen.astype(BF), jnp.where(before, 1.0, 0.0).astype(BF))
        slot = lax.bitwise_and(row, 3).astype(F32)
        placed = jnp.where((chosen > 0.5) & (earlier == slot), 1.0, 0.0)
        combine[...] = placed * weight
        out_tok[...] = dot(placed.astype(BF), tokens[...]).astype(BF).reshape(64, 8, WIDTH)
        arr_s[2 * g] = out_tok[2 * g]
        arr_s[2 * g + 1] = out_tok[2 * g + 1]

    for copy in staged + sum(loads, []) + down_staged + down_loads:
        copy.wait()
    with jax.named_scope("barrier"):
        pl.semaphore_wait(barrier, 70)

    with jax.named_scope("issue"):
        for dy, flip in AWAY:
            px, pg = away(dy, flip)
            if flip & 1:
                pltpu.make_async_remote_copy(
                    out_tok.at[pg * 2 + px], arr_o.at[g], sent, o_recv, **at(z, px, pg)).start()
            else:
                pltpu.make_async_remote_copy(
                    out_tok.at[pl.ds(pg * 2, 2)], arr_s.at[pl.ds(g * 2, 2)], sent, d_recv, **at(z, px, pg)).start()
        for send in sum(sends, []) + down_sends[:SOON]:
            send.start()

    with jax.named_scope("cast"):
        load_td.wait()
        for r in range(16):
            td_send[r // 2, r % 2] = td[:, :, 128 * r : 128 * r + 128].astype(BF)

    def rows_of(r):
        return pl.ds(pl.multiple_of(48 * r, 16), 48)

    def push(src, dst, send_sem, recv_sem, dz):
        pltpu.make_async_remote_copy(src, dst, send_sem, recv_sem, **at(along(dz), xl, g)).start()

    mine, theirs = rows_of(rank), rows_of(z * 2 + other)
    own = [
        pltpu.make_async_copy(td_send.at[z, xl], synced.at[:, mine], load_sem.at[6]),
        pltpu.make_async_copy(combine, shares, load_sem.at[8]),
    ]
    for copy in own:
        copy.start()

    def spread(block, rows, far, send_sem, recv_sem, dz):
        if dz == 4:
            for way in range(2):
                push(block.at[pl.ds(2 * way, 2)], td_far.at[far, way], send_sem, v_recv.at[far], 2 - 4 * way)
        else:
            push(block, synced.at[:, rows], send_sem, recv_sem, dz)

    def passed_on(far, side, send_sem, recv_sem):
        with jax.named_scope(f"wait_v{far}"):
            waited(td_far.at[far], 2, v_recv.at[far]).wait()
        for way in range(2):
            dz = 2 - 4 * way
            push(td_far.at[far, way], synced.at[pl.ds(2 * way, 2), rows_of(along(-dz) * 2 + side)], send_sem, recv_sem, dz)

    for dz in (4, 1, 7, 2, 6, 3, 5):
        spread(td_send.at[along(dz), xl], mine, 0, sent, a_recv, dz)
    across = [
        pltpu.make_async_remote_copy(
            td_send.at[along(dz), other], td_relay.at[along(dz)], sent, x_recv.at[n], **at(z, other, g))
        for n, dz in enumerate(FAR)
    ]

    def waited(buf, n, sem):
        return pltpu.make_async_copy(buf.at[pl.ds(0, n)], buf.at[pl.ds(0, n)], sem)

    passed_on(0, xl, sent, a_recv)
    with jax.named_scope("wait_d"):
        waited(arr_s, 62, d_recv).wait()
        waited(arr_o, 32, o_recv).wait()
    r0 = lax.broadcasted_iota(jnp.int32, (512, 512), 0)
    r1 = lax.broadcasted_iota(jnp.int32, (512, 512), 1)
    pair = lax.bitwise_and(lax.shift_right_logical(r0, 8) + xl, 1)
    source = bits(r0, 2, 31) * 16 + pair * 8 + bits(r0, 7, 1) * 4 + bits(r0, 0, 3)
    x_own = dot(jnp.where(source == r1, 1.0, 0.0).astype(BF), arr_s[...].reshape(512, WIDTH)).astype(BF)

    def grouped(r):
        return bits(r, 2, 31) * 8 + bits(r, 7, 1) * 4 + bits(r, 0, 3)

    r0, r1 = r0[:256, :256], r1[:256, :256]
    order = jnp.where(grouped(r0) == r1, 1.0, 0.0).astype(BF)
    back = jnp.where(grouped(r1) == r0, 1.0, 0.0).astype(BF)
    x_both = jnp.concatenate([x_own[:256], dot(order, arr_o[...].reshape(256, WIDTH)).astype(BF)], axis=1)

    def sign(n):
        return 1 if n % 2 == 0 else -1

    def partial(n):
        width, e = PIECES[n][1:]
        with jax.named_scope(f"wait_w{n}"):
            for copy in sends[n]:
                copy.wait_recv()
        if n == 0:
            for q in range(4):
                psend[0][:, q] = dot(x_own[128 * q : 128 * q + 128], weights[0][q]).astype(BF).reshape(8, 16, 2 * width)
        else:
            psend[n][:, 0] = dot(x_both[128 * e : 128 * e + 128], weights[n][...]).astype(BF).reshape(8, 16, 2 * width)
        if n in STRAIGHT:
            for m, dz in enumerate(ZAWAY):
                push(psend[n].at[along(dz)], precv[n].at[m], sent, p_recv.at[n], dz)
            return
        push(psend[n].at[along(4)], precv[n].at[4], sent, r_recv.at[n], 2 * sign(n))
        push(psend[n].at[along(3)], precv[n].at[2], sent, r_recv.at[n], 1)
        push(psend[n].at[along(-3)], precv[n].at[3], sent, r_recv.at[n], -1)
        push(psend[n].at[along(1)], precv[n].at[0], sent, p_recv.at[n], 1)
        push(psend[n].at[along(-1)], precv[n].at[1], sent, p_recv.at[n], -1)

    def relayed(n):
        if n in STRAIGHT:
            return
        with jax.named_scope(f"wait_r{n}"):
            waited(precv[n], 3, r_recv.at[n]).wait()
        ahead = psend[n][along(2)].astype(F32) + precv[n][2].astype(F32)
        behind = psend[n][along(-2)].astype(F32) + precv[n][3].astype(F32)
        far = precv[n][4].astype(F32)
        if sign(n) > 0:
            ahead = ahead + far
        else:
            behind = behind + far
        pagg[n][0] = ahead.astype(BF)
        pagg[n][1] = behind.astype(BF)
        push(pagg[n].at[0], precv[n].at[5], sent, p_recv.at[n], 2)
        push(pagg[n].at[1], precv[n].at[6], sent, p_recv.at[n], -2)

    def activated(n, total):
        width = PIECES[n][1]
        hid[n][z] = (silu(total[:, :, :width]) * total[:, :, width:]).astype(BF)
        block = hid[n].at[z]
        if n in DIRECT:
            for dz in ZAWAY:
                push(block, block, sent, h_recv.at[n], dz)
        else:
            for dz in (2, -2):
                push(block, block, sent, f_recv.at[n], dz)
            for dz in (1, -1):
                push(block, block, sent, h_recv.at[n], dz)

    halves = pltpu.make_async_remote_copy(half_send, half_recv, sent, half_sem, **at(z, other, g))

    def reduced(n):
        with jax.named_scope(f"wait_p{n}"):
            waited(precv[n], 7 if n in STRAIGHT else 4, p_recv.at[n]).wait()
        total = psend[n][z].astype(F32)
        for s in range(7) if n in STRAIGHT else (0, 1, 5, 6):
            total = total + precv[n][s].astype(F32)
        if n == 0:
            half_send[...] = total[2:].astype(BF)
            half_sum[...] = total[:2]
            halves.start()
            for copy in down_sends[SOON:] + across:
                copy.start()
        else:
            activated(n, total)

    def both_halves(n):
        with jax.named_scope("wait_half"):
            halves.wait_recv()
        activated(n, half_sum[...] + half_recv[...].astype(F32))

    def forwarded(n):
        if n in DIRECT:
            return
        with jax.named_scope(f"wait_f{n}"):
            waited(hid[n], 2, f_recv.at[n]).wait()
        left, right = hid[n].at[along(-2)], hid[n].at[along(2)]
        if sign(n) > 0:
            push(left, left, sent, h_recv.at[n], 2)
        else:
            push(right, right, sent, h_recv.at[n], -2)
        push(left, left, sent, h_recv.at[n], 1)
        push(right, right, sent, h_recv.at[n], -1)

    def hop(n):
        dz = FAR[n]
        with jax.named_scope(f"wait_x{n}"):
            across[n].wait_recv()
        if dz == 0:
            own.append(pltpu.make_async_copy(td_relay.at[z], synced.at[:, theirs], load_sem.at[7]))
            own[-1].start()
        else:
            spread(td_relay.at[along(dz)], theirs, 1, sent, b_recv, dz)

    stages = (partial, relayed, reduced, forwarded, both_halves)
    for step in ORDER:
        stages[step // 10](step % 10)

    for n in range(EARLY):
        hop(n)
    with jax.named_scope("wait_wd"):
        for e in range(2):
            down_sends[e].wait_recv()
    outs = [None, None]
    for n, (first, width, expert) in enumerate(PIECES):
        with jax.named_scope(f"wait_h{n}"):
            waited(hid[n], 7 if n in DIRECT else 5, h_recv.at[n]).wait()
        for m, e in enumerate((0, 1) if n == 0 else (expert,)):
            term = dot(hid[n][:, m].reshape(128, width), wd[e, first : first + width])
            outs[e] = term if outs[e] is None else outs[e] + term
    out = dot(back, jnp.concatenate(outs, axis=0).astype(BF)).astype(BF)
    for n in range(2):
        oute[32 * n : 32 * n + 32] = out[:, WIDTH * n : WIDTH * n + WIDTH].reshape(32, 8, WIDTH)
    own.append(pltpu.make_async_copy(oute.at[g], ret.at[seat], load_sem.at[9]))
    own[-1].start()
    with jax.named_scope("issue_e"):
        for dy, flip in AWAY:
            px, pg = away(dy, flip)
            pltpu.make_async_remote_copy(
                oute.at[(flip & 1) * 32 + pg], ret.at[seat], sent, e_recv, **at(z, px, pg)).start()

    for n in range(EARLY, 8):
        hop(n)
    passed_on(1, other, sent, b_recv)
    with jax.named_scope("wait_e"):
        waited(oute, 63, e_recv).wait()

    with jax.named_scope("wait_a"):
        for copy in own:
            copy.wait()
        for sem in (a_recv, b_recv):
            waited(td_relay, 7, sem).wait()
        for sem in (sent, sent):
            waited(td_relay, 8, sem).wait()
        for copy in across:
            copy.wait_send()
    with jax.named_scope("wait_sends"):
        waited(out_tok, 62, sent).wait()
        waited(out_tok, 32, sent).wait()
        waited(oute, 63, sent).wait()
        halves.wait_send()
        for n in range(count):
            waited(psend[n], 7, sent).wait()
            waited(hid[n], 7, sent).wait()
        for send in sum(sends, []) + down_sends:
            send.wait_send()


def write_out(ret, shares, synced, mixed_out, synced_out, mixed, sem):
    copy = pltpu.make_async_copy(synced, synced_out, sem.at[1])
    copy.start()
    mixed[...] = lax.dot_general(
        shares[...], ret[...].reshape(shares.shape[0], ret.shape[2]).astype(F32), (((0,), (0,)), ((), ())),
        precision=lax.Precision.HIGHEST, preferred_element_type=F32,
    ).astype(BF)
    last = pltpu.make_async_copy(mixed, mixed_out, sem.at[0])
    last.start()
    copy.wait()
    last.wait()


def local(tokens, routes, route_weight, gate, up, down, trained):
    V, A = pl.BlockSpec(memory_space=pltpu.VMEM), pl.BlockSpec(memory_space=pl.ANY)
    FF = gate.shape[2]
    count = len(PIECES)
    wide = [2 * width for _, width, _ in PIECES]

    def vmem(*shape, dtype=BF):
        return pltpu.VMEM(shape, dtype)

    def dma(*shape):
        return pltpu.SemaphoreType.DMA(shape)

    scratch = [
        vmem(*tokens.shape), vmem(8, 32, dtype=jnp.int32), vmem(8, 32, dtype=F32),
        vmem(64, 8, 128), vmem(64, 8, 128), vmem(32, 8, 128), vmem(2, FF, 256), vmem(64, 8, 128),
        vmem(*trained.shape, dtype=F32), vmem(8, 2, 4, 48, 128), vmem(8, 4, 48, 128), vmem(2, 2, 2, 48, 128), vmem(512, 32, dtype=F32),
        vmem(2, 16, wide[0], dtype=F32), vmem(2, 16, wide[0]), vmem(2, 16, wide[0]),
        dma(10), dma(), dma(1 + count), dma(), dma(),
        dma(count), dma(count), dma(count), dma(count),
        dma(), dma(), dma(), dma(8), dma(), dma(), dma(2),
    ]
    scratch += [vmem(*((4, 128, wide[0]) if n == 0 else (256, wide[n]))) for n in range(count)]
    scratch += [vmem(*((2, FF, 128) if n == 0 else (128, wide[n]))) for n in range(count)]
    for devices in (8, 7, 2):
        scratch += [vmem(devices, experts_in(n), 16, wide[n]) for n in range(count)]
    scratch += [vmem(8, 2 if n == 0 else 1, 16, wide[n] // 2) for n in range(count)]
    out = pl.pallas_call(
        kernel,
        out_shape=(pltpu.VMEM((64, 8, 128), BF), pltpu.VMEM((512, 32), F32), pltpu.VMEM(down.shape, BF)),
        in_specs=[A] * 7,
        out_specs=(A, A, A),
        scratch_shapes=scratch,
        compiler_params=pltpu.CompilerParams(collective_id=0, has_side_effects=True),
        name="moe_step",
    )(tokens, routes.T, route_weight.T, gate, up, down, trained)
    out = [pltpu.with_memory_space_constraint(o, pltpu.VMEM) for o in out]
    return pl.pallas_call(
        write_out,
        out_shape=(jax.ShapeDtypeStruct(tokens.shape, BF), jax.ShapeDtypeStruct(down.shape, BF)),
        in_specs=[V, V, V],
        out_specs=(A, A),
        scratch_shapes=[vmem(*tokens.shape), dma(2)],
        name="write_out",
    )(*out)


def solution(mesh):
    torus = Mesh(mesh.devices.reshape(8, 2, mesh.shape["expert"]), ("z", "xl", "expert"))
    placed = (
        P("expert", DP),
        P("expert", None),
        P("expert", None),
        P("expert", DP, None),
        P("expert", DP, None),
        P("expert", None, DP),
        P("expert", DP, None),
    )
    return jax.shard_map(
        local,
        mesh=torus,
        in_specs=placed,
        out_specs=(P("expert", DP), P("expert", None, DP)),
        check_vma=False,
    )
```
